32 devices in a mesh: groups: 2 (over x), seq: 16 (over z, y, core).
Axes of the slice: x: 2, y: 2, z: 4, core: 2. Of those that a mesh axis runs over, the one named last changes fastest.
Arguments:
- queries: bfloat16 [2048, 4096], P(('groups', 'seq')), parts along dimension 0, may hold values from -8 to 8
- keys: bfloat16 [2048, 512], P(('groups', 'seq')), parts along dimension 0, may hold values from -8 to 8
- values: bfloat16 [2048, 512], P(('groups', 'seq')), parts along dimension 0, may hold values from -6 to 6
- block_pairs: int32 [32], P('groups'), parts along dimension 0, may hold values from 0 to 15, each once
- decode_slots: int32 [32], P('groups'), parts along dimension 0, may hold values from 0 to 15, each once
Outputs:
- attended: bfloat16 [2048, 4096], P(('groups', 'seq')), parts along dimension 0
- decode_cache: bfloat16 [32, 256, 2, 128], P(('groups', 'seq')), parts along dimension 0
The draws below stay inside these ranges and needn't reach their ends.
There are 2 independent parts, one for each index of `groups`. The reference program is written for one: setup_inputs(seed, part) draws one part's arguments, and reference() takes and returns one part's arrays. A program takes and returns all parts, laid end to end along the dimension named above; each array names one. Nothing has to cross between parts.
Inputs may be any that keep to these rules, and one draw needn't show every extreme that they name: `block_pairs`: each of 0 to 15 once. `decode_slots`: each of 0 to 15 once.
All inputs are finite; a program needn't handle non-finite values.
Results may differ from the reference program's by a relative error of at most 0.012.
The reference program's roundings to bfloat16 on the way (of `rotated_queries`, `rotated_keys` and `rounded`) count: a program that leaves them out, or rounds other values in their place, can miss the bound.
Values may be sent and summed in bfloat16 or wider, within the bound.
No kernel may reach another device: no remote copies, remote signals or barrier semaphores. Data moves between devices by JAX's collectives and lax.ppermute only.
A program may use at most 128 MiB of HBM per device.

```python
import math
import jax
import jax.numpy as jnp
from jax import lax

HD = 128
KVH = 4
GQ = 8
TOK_DEV = 64
QH = 32
SEQ = 1024
STRIDE = 4
CACHE_LEN = 256
N_SEQ = 16


def joint_draw(key):
    query_base = jnp.clip(jax.random.normal(jax.random.fold_in(key, 101), (SEQ, QH, HD), jnp.float32), -4.0, 4.0)
    key_base = jnp.clip(jax.random.normal(jax.random.fold_in(key, 102), (SEQ, KVH, HD), jnp.float32), -4.0, 4.0)
    return (query_base, key_base)


def draw_queries(key, part):
    query_base, key_base = joint_draw(key)
    return query_base.reshape(SEQ, QH * HD).astype(jnp.bfloat16)


def draw_keys(key, part):
    query_base, key_base = joint_draw(key)
    return key_base.reshape(SEQ, KVH * HD).astype(jnp.bfloat16)


def level_of(own_key, dims, pieces, smallest, largest):
    factor_of, own = 1.0, jax.random.fold_in(own_key, 6)
    for dim, blocks in pieces:
        heights = jnp.exp(jax.random.uniform(jax.random.fold_in(own, dim), (blocks,), jnp.float32, smallest / len(pieces), largest / len(pieces)))
        factor_of = factor_of * jnp.repeat(heights, dims[dim] // blocks).reshape([-1 if axis == dim else 1 for axis in range(len(dims))])
    return factor_of


def gaussian(key, extent, deviation, reach, cuts=(), held_as=jnp.bfloat16):
    result = deviation * jax.random.normal(key, extent, jnp.float32)
    if cuts:
        result = result * level_of(key, extent, cuts, -0.22, 0.18)
    return jnp.clip(result, -reach, reach).astype(held_as)


def setup_inputs(seed: int = 0, part: int = 0) -> dict:
    arg_keys = jax.random.split(jax.random.key(seed), 6)
    own_keys = jax.random.split(jax.random.fold_in(arg_keys[5], part), 6)
    return {
        "queries": draw_queries(jax.random.fold_in(jax.random.fold_in(arg_keys[5], part), 71), part),
        "keys": draw_keys(jax.random.fold_in(jax.random.fold_in(arg_keys[5], part), 71), part),
        "values": gaussian(own_keys[2], (SEQ, KVH * HD), 1.0, 6.0, ((0, 16),)),
        "block_pairs": jax.random.permutation(own_keys[3], N_SEQ).astype(jnp.int32),
        "decode_slots": jax.random.permutation(own_keys[4], N_SEQ).astype(jnp.int32),
    }


ROPE_BASE = 500000.0
NEGATIVE = -1e+30

def rotate_rows(vectors, positions):
    half_dim = vectors.shape[-1] // 2
    frequency = ROPE_BASE ** (-(jnp.arange(half_dim, dtype=jnp.float32) * 2.0) / vectors.shape[-1])
    angles = positions.astype(jnp.float32)[:, None] * frequency[None, :]
    cosine_part = jnp.cos(angles)[:, None, :]
    sine_part = jnp.sin(angles)[:, None, :]
    first_half = vectors[..., :half_dim]
    second_half = vectors[..., half_dim:]
    return jnp.concatenate([first_half * cosine_part - second_half * sine_part, second_half * cosine_part + first_half * sine_part], axis=-1)

def token_positions(block_pairs, tok_dev):
    devices = block_pairs.shape[0]
    half_tok = tok_dev // 2
    within = jnp.arange(tok_dev, dtype=jnp.int32)
    late_flag = (within >= half_tok).astype(jnp.int32)
    block_index = block_pairs[:, None] * (1 - late_flag)[None, :] + (2 * devices - 1 - block_pairs[:, None]) * late_flag[None, :]
    return (block_index * half_tok + (within % half_tok)[None, :]).reshape(-1)

def reference(queries, keys, values, block_pairs, decode_slots):
    positions = token_positions(block_pairs, TOK_DEV)
    rotated_queries = rotate_rows(queries.astype(jnp.float32).reshape(SEQ, QH, HD), positions).astype(jnp.bfloat16)
    rotated_keys = rotate_rows(keys.astype(jnp.float32).reshape(SEQ, KVH, HD), positions).astype(jnp.bfloat16)
    value_rows = values.reshape(SEQ, KVH, HD)
    key_wide = lax.optimization_barrier(rotated_keys).astype(jnp.float32)
    value_wide = value_rows.astype(jnp.float32)
    query_wide = lax.optimization_barrier(rotated_queries).astype(jnp.float32).reshape(SEQ, KVH, GQ, HD)
    score_scale = 1.0 / math.sqrt(HD)

    def one_block(block_index):
        query_rows = lax.dynamic_slice_in_dim(query_wide, block_index * TOK_DEV, TOK_DEV, 0)
        row_pos = lax.dynamic_slice_in_dim(positions, block_index * TOK_DEV, TOK_DEV, 0)
        scores = jnp.einsum('tkgd,ukd->tkgu', query_rows, key_wide) * score_scale
        allowed = (positions[None, :] <= row_pos[:, None])[:, None, None, :]
        maxima = lax.optimization_barrier(jnp.max(jnp.where(allowed, scores, NEGATIVE), axis=-1, keepdims=True))
        weights = jnp.where(allowed, jnp.exp(scores - maxima), 0.0)
        totals = lax.optimization_barrier(jnp.sum(weights, axis=-1))
        rounded = lax.optimization_barrier(weights.astype(jnp.bfloat16)).astype(jnp.float32)
        mixture = jnp.einsum('tkgu,ukd->tkgd', rounded, value_wide)
        return (mixture / totals[..., None]).astype(jnp.bfloat16).reshape(TOK_DEV, QH * HD)
    attended = lax.map(one_block, jnp.arange(N_SEQ, dtype=jnp.int32)).reshape(SEQ, QH * HD)
    row_of_position = jnp.zeros((SEQ,), jnp.int32).at[positions].set(jnp.arange(SEQ, dtype=jnp.int32))
    stacked = jnp.stack([rotated_keys, value_rows], axis=2)
    arranged = stacked[row_of_position].reshape(CACHE_LEN, STRIDE, KVH, 2, HD)
    picked = arranged[:, decode_slots % STRIDE, decode_slots // STRIDE]
    decode_cache = jnp.moveaxis(picked, 1, 0)
    return (attended, decode_cache)
```

```python
import functools
import math

import jax
import jax.numpy as jnp
from jax import lax
from jax.experimental import pallas as pl
from jax.experimental.pallas import tpu as pltpu
from jax.sharding import PartitionSpec as P

HD = 128
KVH = 4
GQ = 8
QH = 32

ROPE_BASE = 500000.0
NEGATIVE = -1e30
LOG2E = math.log2(math.e)

VMEM_SPEC = pl.BlockSpec(memory_space=pltpu.VMEM)
SMEM_SPEC = pl.BlockSpec(memory_space=pltpu.SMEM)
F32 = jnp.float32
BF16 = jnp.bfloat16


def params(mib):
    return pltpu.CompilerParams(vmem_limit_bytes=mib << 20)


def rotation_tables(block, devices, tok_dev):
    half_tok = tok_dev // 2
    row = lax.broadcasted_iota(jnp.int32, (tok_dev, HD), 0)
    lane = lax.broadcasted_iota(jnp.int32, (tok_dev, HD), 1)
    early = row < half_tok
    position = jnp.where(
        early, block * half_tok + row, (2 * devices - 1 - block) * half_tok + row - half_tok
    )
    low = lane < HD // 2
    index = jnp.where(low, lane, lane - HD // 2).astype(F32)
    frequency = jnp.exp(index * (-2.0 * math.log(ROPE_BASE) / HD))
    angle = position.astype(F32) * frequency
    sine = jnp.sin(angle)
    return jnp.cos(angle), jnp.where(low, -sine, sine)


def turn(block, cosine, sine):
    wide = block.astype(F32)
    return (wide * cosine + pltpu.roll(wide, HD // 2, 1) * sine).astype(BF16)


def prep_kernel(devices, pairs_ref, k_ref, v_ref, kv_ref, trig_ref):
    tok_dev = k_ref.shape[0]
    cosine, sine = rotation_tables(pairs_ref[lax.axis_index("seq")], devices, tok_dev)
    for g in range(KVH):
        cols = slice(g * HD, (g + 1) * HD)
        kv_ref[:, cols] = turn(k_ref[:, cols], cosine, sine)
    kv_ref[:, KVH * HD :] = v_ref[...]
    trig_ref[:, :HD] = cosine
    trig_ref[:, HD:] = sine


def prep(pairs, keys, values):
    devices = lax.axis_size("seq")
    tok_dev = keys.shape[0]
    return pl.pallas_call(
        functools.partial(prep_kernel, devices),
        out_shape=(
            jax.ShapeDtypeStruct((tok_dev, 2 * KVH * HD), BF16),
            jax.ShapeDtypeStruct((tok_dev, 2 * HD), F32),
        ),
        in_specs=[SMEM_SPEC, VMEM_SPEC, VMEM_SPEC],
        out_specs=(VMEM_SPEC, VMEM_SPEC),
        compiler_params=params(8),
        name="prep",
    )(pairs, keys, values)


def chunk_kernel(devices, offsets, counts, first, last, *refs):
    refs = list(refs)
    pairs_ref, slots_ref = refs.pop(0), refs.pop(0)
    block_refs = [refs.pop(0) for _ in counts]
    if first:
        q_ref, trig_ref = refs.pop(0), refs.pop(0)
    else:
        turned_ref = refs.pop(0)
        old_refs = [refs.pop(0) for _ in range(3)]
        old_cache_ref = refs.pop(0)
    if first:
        new_turned_ref = refs.pop(0)
        turned_ref = new_turned_ref
    if last:
        out_ref = refs.pop(0)
    else:
        new_refs = [refs.pop(0) for _ in range(3)]
    cache_ref = refs.pop(0)

    me = lax.axis_index("seq")
    own = pairs_ref[me]
    tok_dev = block_refs[0].shape[-2]
    half_tok = tok_dev // 2
    stride = devices // KVH
    peers = len(offsets)
    keys_half = peers * half_tok
    rows = GQ * half_tok

    where = []
    for ref, count in zip(block_refs, counts):
        where += [ref.at[i] for i in range(count)] if count else [ref]
    pair_of = [pairs_ref[lax.bitwise_xor(me, offset)] for offset in offsets]

    lane = lax.broadcasted_iota(jnp.int32, (1, keys_half), 1)
    key_pair = jnp.zeros((1, keys_half), jnp.int32)
    for i, pair in enumerate(pair_of):
        key_pair = jnp.where(lane // half_tok == i, pair, key_pair)
    within = lane % half_tok
    early_pos = key_pair * half_tok + within
    late_pos = (2 * devices - 1 - key_pair) * half_tok + within
    token = lax.broadcasted_iota(jnp.int32, (half_tok, 1), 0)
    early_ok = early_pos <= own * half_tok + token
    late_ok = late_pos <= (2 * devices - 1 - own) * half_tok + token

    if first:
        cosine, sine = trig_ref[:, :HD], trig_ref[:, HD:]
        for head in range(QH):
            turned = turn(q_ref[:, head * HD : (head + 1) * HD], cosine, sine)
            g, r = head // GQ, head % GQ
            for half in range(2):
                turned_ref[half, g, r * half_tok : (r + 1) * half_tok, :] = turned[
                    half * half_tok : (half + 1) * half_tok
                ]

    def gathered(col, half):
        return jnp.concatenate(
            [
                w[half * half_tok : (half + 1) * half_tok, col : col + HD]
                for w in where
            ],
            axis=0,
        )

    contract_last = (((1,), (1,)), ((), ()))
    scale = LOG2E / math.sqrt(HD)

    def masked(scores, allowed):
        grid = scores.reshape(GQ, half_tok, keys_half)
        return jnp.where(allowed[None], grid, NEGATIVE).reshape(rows, keys_half)

    def update(half, g, parts):
        top = parts[0][0]
        for scores, _ in parts[1:]:
            top = jnp.maximum(top, scores)
        top = jnp.max(top, axis=1, keepdims=True)
        if not first:
            old_max = old_refs[0][half, g]
            top = jnp.maximum(old_max[:, :1], top)
            factor = jnp.exp2(old_max[:, :1] - top)
        sums, mixture = None, None
        for scores, value in parts:
            weights = jnp.exp2(scores - top)
            part_sum = weights[:, :HD]
            for start in range(HD, keys_half, HD):
                part_sum = part_sum + weights[:, start : start + HD]
            product = jnp.dot(weights.astype(BF16), value, preferred_element_type=F32)
            sums = part_sum if sums is None else sums + part_sum
            mixture = product if mixture is None else mixture + product
        if not first:
            sums = old_refs[1][half, g] * factor + sums
            mixture = old_refs[2][half, g] * factor + mixture
        if last:
            total = jnp.sum(sums, axis=1, keepdims=True)
            result = (mixture / total).astype(BF16)
            for r in range(GQ):
                head = g * GQ + r
                out_ref[
                    half * half_tok : (half + 1) * half_tok, head * HD : (head + 1) * HD
                ] = result[r * half_tok : (r + 1) * half_tok]
        else:
            new_refs[0][half, g] = jnp.broadcast_to(top, (rows, HD))
            new_refs[1][half, g] = sums
            new_refs[2][half, g] = mixture

    for g in range(KVH):
        key_early, key_late = gathered(g * HD, 0), gathered(g * HD, 1)
        value_early, value_late = gathered((KVH + g) * HD, 0), gathered((KVH + g) * HD, 1)
        query_early, query_late = turned_ref[0, g], turned_ref[1, g]

        def product(query, key):
            return (
                lax.dot_general(query, key, contract_last, preferred_element_type=F32) * scale
            )

        update(0, g, [(masked(product(query_early, key_early), early_ok), value_early)])
        update(
            1,
            g,
            [
                (product(query_late, key_early), value_early),
                (masked(product(query_late, key_late), late_ok), value_late),
            ],
        )

    slot = slots_ref[me]
    head = slot // stride
    phase = slot % stride
    cache_rows = cache_ref.shape[0]
    row = lax.broadcasted_iota(jnp.int32, (cache_rows, 1), 0)
    target = (row // 2) * stride + phase
    key_target = jnp.where(row % 2 == 0, target, -1)
    value_target = jnp.where(row % 2 == 1, target, -1)
    key_col = pl.multiple_of(head * HD, HD)
    value_col = pl.multiple_of((KVH + head) * HD, HD)
    total = None
    for half, pos in ((0, early_pos), (1, late_pos)):
        for col, wanted in ((key_col, key_target), (value_col, value_target)):
            data = jnp.concatenate(
                [w[half * half_tok : (half + 1) * half_tok, pl.ds(col, HD)] for w in where], axis=0
            )
            pick = jnp.where(pos == wanted, 1.0, 0.0).astype(BF16)
            part = jnp.dot(pick, data, preferred_element_type=F32)
            total = part if total is None else total + part
    if not first:
        total = total + old_cache_ref[...].astype(F32)
    cache_ref[...] = total.astype(BF16)


def attend_chunk(pairs, slots, blocks, offsets, counts, queries, trig, state, last):
    devices = lax.axis_size("seq")
    tok_dev = blocks[0].shape[-2]
    stride = devices // KVH
    cache_rows = 2 * tok_dev * devices // stride
    rows = GQ * tok_dev // 2
    first = state is None
    operands = [pairs, slots, *blocks]
    operands += [queries, trig] if first else list(state)
    part = jax.ShapeDtypeStruct((2, KVH, rows, HD), F32)
    outs = []
    if first:
        outs.append(jax.ShapeDtypeStruct((2, KVH, rows, HD), BF16))
    if last:
        outs.append(jax.ShapeDtypeStruct((tok_dev, QH * HD), BF16))
    else:
        outs += [part] * 3
    outs.append(jax.ShapeDtypeStruct((cache_rows, HD), BF16))
    aliases = {}
    base = 2 + len(blocks)
    if not first:
        if not last:
            aliases = {base + 1: 0, base + 2: 1, base + 3: 2, base + 4: 3}
        else:
            aliases = {base + 4: 1}
    results = pl.pallas_call(
        functools.partial(chunk_kernel, devices, offsets, counts, first, last),
        out_shape=tuple(outs),
        in_specs=[SMEM_SPEC, SMEM_SPEC] + [VMEM_SPEC] * (len(operands) - 2),
        out_specs=tuple([VMEM_SPEC] * len(outs)),
        input_output_aliases=aliases,
        compiler_params=params(24),
        name="attend",
    )(*operands)
    if first:
        return tuple(results)
    if last:
        return results
    return (state[0], *results)


def shards(queries, keys, values, block_pairs, decode_slots):
    devices = lax.axis_size("seq")
    tok_dev = queries.shape[0]
    stride = devices // KVH
    cores = 2
    chips = devices // cores
    outer = 1 << -(-(chips.bit_length() - 1) // 2)
    inner = chips // outer

    def swap(x, offset):
        return lax.ppermute(x, "seq", [(s, s ^ offset) for s in range(devices)])

    kv, trig = prep(block_pairs, keys, values)
    plane = inner * cores
    far = [kv] + [swap(kv, step * plane) for step in range(1, outer)]
    order = [0] + list(range(1, outer))
    state, result = None, None
    for place, step in enumerate(order):
        block = far[step]
        near = [block] + [swap(block, y * cores) for y in range(1, inner)]
        pair = swap(jnp.stack(near), 1)
        blocks = near + [pair]
        base = step * plane
        offsets = tuple(
            [base + y * cores for y in range(inner)] + [base + y * cores + 1 for y in range(inner)]
        )
        counts = tuple([0] * inner + [inner])
        state = attend_chunk(
            block_pairs,
            decode_slots,
            blocks,
            offsets,
            counts,
            queries,
            trig,
            state,
            place == outer - 1,
        )
    attended, cache = state
    return attended, cache.reshape(1, tok_dev * devices // stride, 2, HD)


def solution(mesh):
    placed = (
        P(("groups", "seq"), None),
        P(("groups", "seq"), None),
        P(("groups", "seq"), None),
        P("groups"),
        P("groups"),
    )
    return jax.shard_map(
        shards,
        mesh=mesh,
        in_specs=placed,
        out_specs=(P(("groups", "seq"), None), P(("groups", "seq"), None, None, None)),
        check_vma=False,
    )
```

```python
import functools
import math

import jax
import jax.numpy as jnp
from jax import lax
from jax.experimental import pallas as pl
from jax.experimental.pallas import tpu as pltpu
from jax.sharding import PartitionSpec as P


HD = 128
KVH = 4
GQ = 8
QH = 32

ROPE_BASE = 500000.0
NEGATIVE = -1e30
LOG2E = math.log2(math.e)

VMEM_SPEC = pl.BlockSpec(memory_space=pltpu.VMEM)
SMEM_SPEC = pl.BlockSpec(memory_space=pltpu.SMEM)
HBM_SPEC = pl.BlockSpec(memory_space=pltpu.HBM)
F32 = jnp.float32
BF16 = jnp.bfloat16


def params(mib):
    return pltpu.CompilerParams(vmem_limit_bytes=mib << 20)


def rotation_tables(block, devices, tok_dev):
    half_tok = tok_dev // 2
    row = lax.broadcasted_iota(jnp.int32, (tok_dev, HD), 0)
    lane = lax.broadcasted_iota(jnp.int32, (tok_dev, HD), 1)
    early = row < half_tok
    position = jnp.where(
        early, block * half_tok + row, (2 * devices - 1 - block) * half_tok + row - half_tok
    )
    low = lane < HD // 2
    index = jnp.where(low, lane, lane - HD // 2).astype(F32)
    frequency = jnp.exp(index * (-2.0 * math.log(ROPE_BASE) / HD))
    angle = position.astype(F32) * frequency
    sine = jnp.sin(angle)
    return jnp.cos(angle), jnp.where(low, -sine, sine)


def turn(block, cosine, sine):
    wide = block.astype(F32)
    return (wide * cosine + pltpu.roll(wide, HD // 2, 1) * sine).astype(BF16)


def prep_kernel(devices, pairs_hbm, k_hbm, v_hbm, kv_ref, trig_ref, pairs_ref, k_ref, sems):
    tok_dev = k_ref.shape[0]
    width = KVH * HD
    pairs_copy = pltpu.make_async_copy(pairs_hbm, pairs_ref, sems.at[0])
    key_copy = pltpu.make_async_copy(k_hbm, k_ref, sems.at[1])
    value_copy = pltpu.make_async_copy(v_hbm, kv_ref.at[:, width:], sems.at[2])
    pairs_copy.start()
    key_copy.start()
    value_copy.start()
    pairs_copy.wait()
    cosine, sine = rotation_tables(pairs_ref[lax.axis_index("seq")], devices, tok_dev)
    trig_ref[:, :HD] = cosine
    trig_ref[:, HD:] = sine
    key_copy.wait()
    for g in range(KVH):
        cols = slice(g * HD, (g + 1) * HD)
        kv_ref[:, cols] = turn(k_ref[:, cols], cosine, sine)
    value_copy.wait()


def prep(pairs, keys, values):
    devices = lax.axis_size("seq")
    tok_dev = keys.shape[0]
    return pl.pallas_call(
        functools.partial(prep_kernel, devices),
        out_shape=(
            jax.ShapeDtypeStruct((tok_dev, 2 * KVH * HD), BF16),
            jax.ShapeDtypeStruct((tok_dev, 2 * HD), F32),
        ),
        in_specs=[HBM_SPEC] * 3,
        out_specs=(VMEM_SPEC, VMEM_SPEC),
        scratch_shapes=[
            pltpu.SMEM((pairs.shape[0],), jnp.int32),
            pltpu.VMEM(keys.shape, BF16),
            pltpu.SemaphoreType.DMA((3,)),
        ],
        compiler_params=params(8),
        name="prep",
    )(pairs, keys, values)


def chunk_kernel(devices, offsets, counts, first, last, *refs):
    refs = list(refs)
    pairs_ref, slots_ref = refs.pop(0), refs.pop(0)
    block_refs = [refs.pop(0) for _ in counts]
    if first:
        q_ref, trig_ref = refs.pop(0), refs.pop(0)
    else:
        turned_ref = refs.pop(0)
        old_refs = [refs.pop(0) for _ in range(3)]
        old_cache_ref = refs.pop(0)
    if first:
        turned_ref = refs.pop(0)
    if last:
        out_ref = refs.pop(0)
    else:
        new_refs = [refs.pop(0) for _ in range(3)]
    cache_ref = refs.pop(0)

    me = lax.axis_index("seq")
    own = pairs_ref[me]
    tok_dev = block_refs[0].shape[-2]
    half_tok = tok_dev // 2
    stride = devices // KVH
    rows = GQ * half_tok

    where = []
    for ref, count in zip(block_refs, counts):
        where += [ref.at[i] for i in range(count)] if count else [ref]
    pair_of = [pairs_ref[lax.bitwise_xor(me, offset)] for offset in offsets]

    if first:
        cosine, sine = trig_ref[:, :HD], trig_ref[:, HD:]
        for g in range(KVH):
            turned = [
                turn(q_ref[:, head * HD : (head + 1) * HD], cosine, sine)
                for head in range(g * GQ, (g + 1) * GQ)
            ]
            for half in range(2):
                part = [t[half * half_tok : (half + 1) * half_tok] for t in turned]
                turned_ref[half, g] = jnp.concatenate(part, axis=0).T

    def gathered(col, half):
        return jnp.concatenate(
            [w[half * half_tok : (half + 1) * half_tok, pl.ds(col, HD)] for w in where], axis=0
        )

    scale = LOG2E / math.sqrt(HD)
    keys_half = len(where) * half_tok

    row = lax.broadcasted_iota(jnp.int32, (half_tok, HD), 0)
    lane = lax.broadcasted_iota(jnp.int32, (half_tok, HD), 1)

    def key_flags(distance):
        column = jnp.where(distance == 0, row, jnp.where(distance < 0, half_tok, HD))
        return jnp.where(lane == column, 1.0, 0.0).astype(BF16)

    early_flags = jnp.concatenate([key_flags(own - pair) for pair in pair_of], axis=0)
    late_flags = jnp.concatenate([key_flags(pair - own) for pair in pair_of], axis=0)
    blank = jnp.zeros((keys_half, HD), BF16)
    order = lax.broadcasted_iota(jnp.int32, (HD, rows), 0)
    token = lax.broadcasted_iota(jnp.int32, (HD, rows), 1) % half_tok
    barred = jnp.where((order > token) & (order <= half_tok), NEGATIVE, 0.0).astype(BF16)
    ones = jnp.ones((16, 2 * keys_half), BF16)

    def scores_of(g):
        key_early, key_late = gathered(g * HD, 0), gathered(g * HD, 1)
        query_early = jnp.concatenate([turned_ref[0, g], barred], axis=0)
        query_late = jnp.concatenate([turned_ref[1, g], barred], axis=0)
        early = jnp.dot(
            jnp.concatenate([key_early, early_flags], axis=1),
            query_early,
            preferred_element_type=F32,
        )
        late_keys = jnp.concatenate([key_early, key_late], axis=0)
        flags = jnp.concatenate([blank, late_flags], axis=0)
        late = jnp.dot(
            jnp.concatenate([late_keys, flags], axis=1), query_late, preferred_element_type=F32
        )
        return early, late

    def update(half, g, scores, values):
        index = half * KVH + g
        top = jnp.max(scores, axis=0, keepdims=True) * scale
        if not first:
            old_max = old_refs[0][index : index + 1, :]
            top = jnp.maximum(old_max, top)
            factor = jnp.exp2(old_max - top)
        weights = jnp.exp2(scores * scale - top).astype(BF16)
        both = jnp.dot(values, weights, preferred_element_type=F32)
        mixture, sums = both[:HD], both[HD : HD + 1]
        if not first:
            sums = old_refs[1][index : index + 1, :] * factor + sums
            mixture = old_refs[2][half, g] * factor + mixture
        if last:
            result = (mixture * (1.0 / sums)).astype(BF16).T
            for r in range(GQ):
                head = g * GQ + r
                out_ref[
                    half * half_tok : (half + 1) * half_tok, head * HD : (head + 1) * HD
                ] = result[r * half_tok : (r + 1) * half_tok]
        else:
            new_refs[0][index : index + 1, :] = top
            new_refs[1][index : index + 1, :] = sums
            new_refs[2][half, g] = mixture

    scores = scores_of(0)
    for g in range(KVH):
        upcoming = scores_of(g + 1) if g + 1 < KVH else None
        value_rows = jnp.concatenate(
            [gathered((KVH + g) * HD, 0), gathered((KVH + g) * HD, 1)], axis=0
        )
        values = jnp.concatenate([value_rows.T, ones], axis=0)
        update(0, g, scores[0], values[:, :keys_half])
        update(1, g, scores[1], values)
        scores = upcoming

    slot = slots_ref[me]
    head = slot // stride
    phase = slot % stride
    per_block = half_tok // stride
    peers = len(where)
    out_rows = 2 * per_block * peers
    row = lax.broadcasted_iota(jnp.int32, (out_rows, peers * half_tok), 0)
    lane = lax.broadcasted_iota(jnp.int32, (out_rows, peers * half_tok), 1)
    source = (row // (2 * per_block)) * half_tok + (row % (2 * per_block)) // 2 * stride + phase
    hit = source == lane
    pick_key = jnp.where(hit & (row % 2 == 0), 1.0, 0.0).astype(BF16)
    pick_value = jnp.where(hit & (row % 2 == 1), 1.0, 0.0).astype(BF16)
    key_col = pl.multiple_of(head * HD, HD)
    value_col = pl.multiple_of((KVH + head) * HD, HD)
    if not first:
        cache_ref[...] = old_cache_ref[...]
    for half in range(2):
        picked = jnp.dot(pick_key, gathered(key_col, half), preferred_element_type=F32)
        picked += jnp.dot(pick_value, gathered(value_col, half), preferred_element_type=F32)
        picked = picked.astype(BF16)
        for i, pair in enumerate(pair_of):
            block = pair if half == 0 else 2 * devices - 1 - pair
            cache_ref[block] = picked[i * 2 * per_block : (i + 1) * 2 * per_block]


def attend_chunk(pairs, slots, blocks, offsets, counts, queries, trig, state, last):
    devices = lax.axis_size("seq")
    tok_dev = blocks[0].shape[-2]
    stride = devices // KVH
    rows = GQ * tok_dev // 2
    first = state is None
    operands = [pairs, slots, *blocks]
    operands += [queries, trig] if first else list(state)
    outs = []
    if first:
        outs.append(jax.ShapeDtypeStruct((2, KVH, HD, rows), BF16))
    if last:
        outs.append(jax.ShapeDtypeStruct((tok_dev, QH * HD), BF16))
    else:
        outs += [jax.ShapeDtypeStruct((2 * KVH, rows), F32)] * 2
        outs.append(jax.ShapeDtypeStruct((2, KVH, HD, rows), F32))
    outs.append(jax.ShapeDtypeStruct((2 * devices, tok_dev // stride, HD), BF16))
    aliases = {}
    base = 2 + len(blocks)
    if not first:
        aliases = {base + 4: 1} if last else {base + 1 + i: i for i in range(4)}
    results = pl.pallas_call(
        functools.partial(chunk_kernel, devices, offsets, counts, first, last),
        out_shape=tuple(outs),
        in_specs=[SMEM_SPEC, SMEM_SPEC] + [VMEM_SPEC] * (len(operands) - 2),
        out_specs=tuple([VMEM_SPEC] * len(outs)),
        input_output_aliases=aliases,
        compiler_params=params(24),
        cost_estimate=pl.CostEstimate(
            flops=6 * len(offsets) * (tok_dev // 2) * rows * KVH * HD * 2 // 1,
            bytes_accessed=1 << 20,
            transcendentals=0,
        ),
        name="attend",
    )(*operands)
    if first or last:
        return tuple(results)
    return (state[0], *results)


def swap(x, offset):
    devices = lax.axis_size("seq")
    return lax.ppermute(x, "seq", [(s, s ^ offset) for s in range(devices)])


def layout_of(devices):
    cores = 2
    chips = devices // cores
    outer = 1 << -(-(chips.bit_length() - 1) // 2)
    return outer, chips // outer, cores


def whole_step(queries, keys, values, block_pairs, decode_slots):
    devices = lax.axis_size("seq")
    tok_dev = queries.shape[0]
    stride = devices // KVH
    outer, inner, cores = layout_of(devices)

    def hbm(x):
        return pltpu.with_memory_space_constraint(x, pltpu.HBM)

    kv, trig = prep(hbm(block_pairs), hbm(keys), hbm(values))
    plane = inner * cores
    far = [kv] + [swap(kv, step * plane) for step in range(1, outer)]
    chunks = []
    for step in range(outer):
        near = [far[step]]
        for y in range(1, inner):
            near.append(swap(far[step], y * cores))
        pair = swap(jnp.stack(near), 1)
        offsets = tuple(
            step * plane + y * cores + core for core in range(cores) for y in range(inner)
        )
        chunks.append((near + [pair], offsets, tuple([0] * inner + [inner])))
    groups = [chunks[:1], chunks[1:-1], chunks[-1:]]
    state = None
    for index, group in enumerate(groups):
        state = attend_chunk(
            block_pairs,
            decode_slots,
            [block for chunk in group for block in chunk[0]],
            tuple(offset for chunk in group for offset in chunk[1]),
            tuple(count for chunk in group for count in chunk[2]),
            queries,
            trig,
            state,
            index == len(groups) - 1,
        )
    attended, cache = state
    return attended, cache.reshape(1, tok_dev * devices // stride, 2, HD)


def solution(mesh):
    placed = (
        P(("groups", "seq"), None),
        P(("groups", "seq"), None),
        P(("groups", "seq"), None),
        P("groups"),
        P("groups"),
    )
    return jax.shard_map(
        whole_step,
        mesh=mesh,
        in_specs=placed,
        out_specs=(P(("groups", "seq"), None), P(("groups", "seq"), None, None, None)),
        check_vma=False,
    )
```

```python
import functools
import math

import jax
import jax.numpy as jnp
from jax import lax
from jax.experimental import pallas as pl
from jax.experimental.pallas import tpu as pltpu
from jax.sharding import PartitionSpec as P


HD = 128
KVH = 4
GQ = 8
QH = 32

ROPE_BASE = 500000.0
NEGATIVE = -1e30
LOG2E = math.log2(math.e)

VMEM_SPEC = pl.BlockSpec(memory_space=pltpu.VMEM)
HBM_SPEC = pl.BlockSpec(memory_space=pltpu.HBM)
F32 = jnp.float32
BF16 = jnp.bfloat16


def params(mib):
    return pltpu.CompilerParams(vmem_limit_bytes=mib << 20)


def rotation_tables(block, devices, tok_dev):
    half_tok = tok_dev // 2
    row = lax.broadcasted_iota(jnp.int32, (tok_dev, HD), 0)
    lane = lax.broadcasted_iota(jnp.int32, (tok_dev, HD), 1)
    early = row < half_tok
    position = jnp.where(
        early, block * half_tok + row, (2 * devices - 1 - block) * half_tok + row - half_tok
    )
    low = lane < HD // 2
    index = jnp.where(low, lane, lane - HD // 2).astype(F32)
    frequency = jnp.exp(index * (-2.0 * math.log(ROPE_BASE) / HD))
    angle = position.astype(F32) * frequency
    sine = jnp.sin(angle)
    return jnp.cos(angle), jnp.where(low, -sine, sine)


def turn(block, cosine, sine):
    wide = block.astype(F32)
    return (wide * cosine + pltpu.roll(wide, HD // 2, 1) * sine).astype(BF16)


def prep_kernel(
    devices, pairs_hbm, slots_hbm, k_hbm, v_hbm, kv_ref, trig_ref, info_ref, pairs_ref, slots_ref, k_ref, sems
):
    tok_dev = k_ref.shape[0]
    width = KVH * HD
    stride = devices // KVH
    copies = [
        pltpu.make_async_copy(pairs_hbm, pairs_ref, sems.at[0]),
        pltpu.make_async_copy(k_hbm, k_ref, sems.at[1]),
        pltpu.make_async_copy(v_hbm, kv_ref.at[:, width:], sems.at[2]),
        pltpu.make_async_copy(slots_hbm, slots_ref, sems.at[3]),
    ]
    for copy in copies:
        copy.start()
    me = lax.axis_index("seq")
    copies[0].wait()
    cosine, sine = rotation_tables(pairs_ref[me], devices, tok_dev)
    trig_ref[:, :HD] = cosine
    trig_ref[:, HD:] = sine
    copies[1].wait()
    for g in range(KVH):
        cols = slice(g * HD, (g + 1) * HD)
        kv_ref[:, cols] = turn(k_ref[:, cols], cosine, sine)
    lane = lax.broadcasted_iota(jnp.int32, (1, devices), 1)
    peers = jnp.zeros((1, devices), jnp.int32)
    for i in range(devices):
        peers = jnp.where(lane == i, pairs_ref[lax.bitwise_xor(me, i)], peers)
    copies[3].wait()
    slot = slots_ref[me]
    info_ref[0:1, :] = peers
    info_ref[1:2, :] = jnp.where(lane == 0, slot // stride, slot % stride)
    copies[2].wait()


def prep(pairs, slots, keys, values):
    devices = lax.axis_size("seq")
    tok_dev = keys.shape[0]
    return pl.pallas_call(
        functools.partial(prep_kernel, devices),
        out_shape=(
            jax.ShapeDtypeStruct((tok_dev, 2 * KVH * HD), BF16),
            jax.ShapeDtypeStruct((tok_dev, 2 * HD), F32),
            jax.ShapeDtypeStruct((2, devices), jnp.int32),
        ),
        in_specs=[HBM_SPEC] * 4,
        out_specs=(VMEM_SPEC,) * 3,
        scratch_shapes=[
            pltpu.SMEM(pairs.shape, jnp.int32),
            pltpu.SMEM(slots.shape, jnp.int32),
            pltpu.VMEM(keys.shape, BF16),
            pltpu.SemaphoreType.DMA((4,)),
        ],
        compiler_params=params(8),
        name="prep",
    )(pairs, slots, keys, values)


def turn_kernel(q_hbm, trig_ref, turned_ref, q_ref, sems):
    tok_dev = q_ref.shape[0]
    half_tok = tok_dev // 2
    width = GQ * HD
    copies = []
    for g in range(KVH):
        cols = pl.ds(g * width, width)
        copies.append(pltpu.make_async_copy(q_hbm.at[:, cols], q_ref.at[:, cols], sems.at[g]))
        copies[g].start()
    cosine, sine = trig_ref[:, :HD], trig_ref[:, HD:]
    for g in range(KVH):
        copies[g].wait()
        turned = [
            turn(q_ref[:, head * HD : (head + 1) * HD], cosine, sine)
            for head in range(g * GQ, (g + 1) * GQ)
        ]
        for half in range(2):
            part = [t[half * half_tok : (half + 1) * half_tok] for t in turned]
            turned_ref[half, g] = jnp.concatenate(part, axis=0).T


def turn_queries(queries, trig):
    rows = GQ * queries.shape[0] // 2
    return pl.pallas_call(
        turn_kernel,
        out_shape=jax.ShapeDtypeStruct((2, KVH, HD, rows), BF16),
        in_specs=[HBM_SPEC, VMEM_SPEC],
        out_specs=VMEM_SPEC,
        scratch_shapes=[pltpu.VMEM(queries.shape, BF16), pltpu.SemaphoreType.DMA((KVH,))],
        compiler_params=params(8),
        name="turn",
    )(queries, trig)


def fold(x):
    return x.reshape(x.shape[0] // 8, 8, x.shape[1])


def spread_max(x):
    for shift in (4, 2, 1):
        x = jnp.maximum(x, pltpu.roll(x, shift, 0))
    return x


def chunk_kernel(devices, offsets, counts, first, last, *refs):
    refs = list(refs)
    info_ref, turned_ref = refs.pop(0), refs.pop(0)
    block_refs = [refs.pop(0) for _ in counts]
    if not first:
        old_refs = [refs.pop(0) for _ in range(3)]
        old_cache_ref = refs.pop(0)
    if last:
        out_hbm, cache_hbm, out_ref, cache_ref, sems = refs
    else:
        new_refs = [refs.pop(0) for _ in range(3)]
        cache_ref = refs.pop(0)

    own = info_ref[0, 0]
    head, phase = info_ref[1, 0], info_ref[1, 1]
    tok_dev = block_refs[0].shape[-2]
    half_tok = tok_dev // 2
    stride = devices // KVH
    rows = GQ * half_tok

    where = []
    for ref, count in zip(block_refs, counts):
        where += [ref.at[i] for i in range(count)] if count else [ref]
    pair_of = [info_ref[0, offset] for offset in offsets]

    def gathered(col, half):
        return jnp.concatenate(
            [w[half * half_tok : (half + 1) * half_tok, pl.ds(col, HD)] for w in where], axis=0
        )

    per_block = half_tok // stride
    peers = len(where)
    out_rows = 2 * per_block * peers
    row = lax.broadcasted_iota(jnp.int32, (out_rows, peers * half_tok), 0)
    lane = lax.broadcasted_iota(jnp.int32, (out_rows, peers * half_tok), 1)
    source = (row // (2 * per_block)) * half_tok + (row % (2 * per_block)) // 2 * stride + phase
    hit = source == lane
    pick_key = jnp.where(hit & (row % 2 == 0), 1.0, 0.0).astype(BF16)
    pick_value = jnp.where(hit & (row % 2 == 1), 1.0, 0.0).astype(BF16)
    key_col = pl.multiple_of(head * HD, HD)
    value_col = pl.multiple_of((KVH + head) * HD, HD)
    if not first:
        cache_ref[...] = old_cache_ref[...]
    for half in range(2):
        picked = jnp.dot(pick_key, gathered(key_col, half), preferred_element_type=F32)
        picked += jnp.dot(pick_value, gathered(value_col, half), preferred_element_type=F32)
        picked = picked.astype(BF16)
        for i, pair in enumerate(pair_of):
            block = pair if half == 0 else 2 * devices - 1 - pair
            cache_ref[block] = picked[i * 2 * per_block : (i + 1) * 2 * per_block]
    copies = []
    if last:
        copies.append(pltpu.make_async_copy(cache_ref, cache_hbm, sems.at[KVH]))
        copies[0].start()

    scale = LOG2E / math.sqrt(HD)
    keys_half = len(where) * half_tok

    row = lax.broadcasted_iota(jnp.int32, (half_tok, HD), 0)
    lane = lax.broadcasted_iota(jnp.int32, (half_tok, HD), 1)

    def key_flags(distance):
        column = jnp.where(distance == 0, row, jnp.where(distance < 0, half_tok, HD))
        return jnp.where(lane == column, 1.0, 0.0).astype(BF16)

    early_flags = jnp.concatenate([key_flags(own - pair) for pair in pair_of], axis=0)
    late_flags = jnp.concatenate([key_flags(pair - own) for pair in pair_of], axis=0)
    blank = jnp.zeros((keys_half, HD), BF16)
    order = lax.broadcasted_iota(jnp.int32, (HD, rows), 0)
    token = lax.broadcasted_iota(jnp.int32, (HD, rows), 1) % half_tok
    barred = jnp.where((order > token) & (order <= half_tok), NEGATIVE, 0.0).astype(BF16)
    ones = jnp.ones((16, 2 * keys_half), BF16)

    def scores_of(g):
        key_early, key_late = gathered(g * HD, 0), gathered(g * HD, 1)
        query_early = jnp.concatenate([turned_ref[0, g], barred], axis=0)
        query_late = jnp.concatenate([turned_ref[1, g], barred], axis=0)
        early = jnp.dot(
            jnp.concatenate([key_early, early_flags], axis=1),
            query_early,
            preferred_element_type=F32,
        )
        late_keys = jnp.concatenate([key_early, key_late], axis=0)
        flags = jnp.concatenate([blank, late_flags], axis=0)
        late = jnp.dot(
            jnp.concatenate([late_keys, flags], axis=1), query_late, preferred_element_type=F32
        )
        return early, late

    def update(half, g, scores, values):
        index = half * KVH + g
        scores = fold(scores)
        top = spread_max(jnp.max(scores, axis=0)) * scale
        if not first:
            old_max = old_refs[0][index]
            top = jnp.maximum(old_max, top)
            factor = jnp.exp2(old_max - top)
        weights = jnp.exp2(scores * scale - top[None]).astype(BF16).reshape(-1, rows)
        both = jnp.dot(values, weights, preferred_element_type=F32)
        mixture, sums = fold(both[:HD]), both[HD : HD + 8]
        if not first:
            sums = old_refs[1][index] * factor + sums
            mixture = fold(old_refs[2][half, g]) * factor[None] + mixture
        if last:
            result = (mixture * (1.0 / sums)[None]).reshape(HD, rows).astype(BF16).T
            for r in range(GQ):
                col = (g * GQ + r) * HD
                out_ref[half * half_tok : (half + 1) * half_tok, col : col + HD] = result[
                    r * half_tok : (r + 1) * half_tok
                ]
        else:
            new_refs[0][index] = top
            new_refs[1][index] = sums
            new_refs[2][half, g] = mixture.reshape(HD, rows)

    scores = [scores_of(g) for g in range(KVH)]
    values = []
    for g in range(KVH):
        value_rows = jnp.concatenate(
            [gathered((KVH + g) * HD, 0), gathered((KVH + g) * HD, 1)], axis=0
        )
        values.append(jnp.concatenate([value_rows.T, ones], axis=0))
    for g in range(KVH):
        update(0, g, scores[g][0], values[g][:, :keys_half])
        update(1, g, scores[g][1], values[g])
        if last:
            cols = pl.ds(g * GQ * HD, GQ * HD)
            copies.append(
                pltpu.make_async_copy(out_ref.at[:, cols], out_hbm.at[:, cols], sems.at[g])
            )
            copies[-1].start()
    for copy in copies:
        copy.wait()


def attend_chunk(info, turned, blocks, offsets, counts, state, last):
    devices = lax.axis_size("seq")
    tok_dev = blocks[0].shape[-2]
    stride = devices // KVH
    rows = GQ * tok_dev // 2
    first = state is None
    operands = [info, turned, *blocks, *(state or ())]
    cache = jax.ShapeDtypeStruct((2 * devices, tok_dev // stride, HD), BF16)
    aliases, scratch = {}, []
    if last:
        out = jax.ShapeDtypeStruct((tok_dev, QH * HD), BF16)
        outs = (out, cache)
        scratch = [
            pltpu.VMEM(out.shape, BF16),
            pltpu.VMEM(cache.shape, BF16),
            pltpu.SemaphoreType.DMA((KVH + 1,)),
        ]
    else:
        small = jax.ShapeDtypeStruct((2 * KVH, 8, rows), F32)
        outs = (small, small, jax.ShapeDtypeStruct((2, KVH, HD, rows), F32), cache)
        if not first:
            aliases = {2 + len(blocks) + i: i for i in range(4)}
    work = len(offsets) * (tok_dev // 2) * rows * KVH * HD
    return pl.pallas_call(
        functools.partial(chunk_kernel, devices, offsets, counts, first, last),
        out_shape=outs,
        in_specs=[VMEM_SPEC] * len(operands),
        out_specs=tuple([HBM_SPEC if last else VMEM_SPEC] * len(outs)),
        scratch_shapes=scratch,
        input_output_aliases=aliases,
        compiler_params=params(24),
        cost_estimate=pl.CostEstimate(flops=12 * work, bytes_accessed=1 << 20, transcendentals=0),
        name="attend",
    )(*operands)


def swap(x, offset):
    devices = lax.axis_size("seq")
    return lax.ppermute(x, "seq", [(s, s ^ offset) for s in range(devices)])


def layout_of(devices):
    cores = 2
    chips = devices // cores
    outer = 1 << -(-(chips.bit_length() - 1) // 2)
    return outer, chips // outer, cores


def whole_step(queries, keys, values, block_pairs, decode_slots):
    devices = lax.axis_size("seq")
    tok_dev = queries.shape[0]
    stride = devices // KVH
    outer, inner, cores = layout_of(devices)

    def hbm(x):
        return pltpu.with_memory_space_constraint(x, pltpu.HBM)

    kv, trig, info = prep(hbm(block_pairs), hbm(decode_slots), hbm(keys), hbm(values))
    turned = turn_queries(hbm(queries), trig)
    plane = inner * cores
    far = [kv] + [swap(kv, step * plane) for step in range(1, outer)]
    chunks = []
    for step in range(outer):
        near = [far[step]]
        for y in range(1, inner):
            near.append(swap(far[step], y * cores))
        pair = swap(jnp.stack(near), 1)
        offsets = tuple(
            step * plane + y * cores + core for core in range(cores) for y in range(inner)
        )
        chunks.append((near + [pair], offsets, tuple([0] * inner + [inner])))
    state = None
    for step, (blocks, offsets, counts) in enumerate(chunks):
        state = attend_chunk(info, turned, blocks, offsets, counts, state, step == outer - 1)
    attended, cache = state
    return attended, cache.reshape(1, tok_dev * devices // stride, 2, HD)


def solution(mesh):
    placed = (
        P(("groups", "seq"), None),
        P(("groups", "seq"), None),
        P(("groups", "seq"), None),
        P("groups"),
        P("groups"),
    )
    return jax.shard_map(
        whole_step,
        mesh=mesh,
        in_specs=placed,
        out_specs=(P(("groups", "seq"), None), P(("groups", "seq"), None, None, None)),
        check_vma=False,
    )
```

```python
import functools
import math

import jax
import jax.numpy as jnp
from jax import lax
from jax.experimental import pallas as pl
from jax.experimental.pallas import tpu as pltpu
from jax.sharding import PartitionSpec as P


HD = 128
KVH = 4
GQ = 8
QH = 32

ROPE_BASE = 500000.0
NEGATIVE = -1e30
LOG2E = math.log2(math.e)

VMEM_SPEC = pl.BlockSpec(memory_space=pltpu.VMEM)
HBM_SPEC = pl.BlockSpec(memory_space=pltpu.HBM)
F32 = jnp.float32
BF16 = jnp.bfloat16


def params(mib):
    return pltpu.CompilerParams(vmem_limit_bytes=mib << 20)


def rotation_tables(block, devices, tok_dev):
    half_tok = tok_dev // 2
    row = lax.broadcasted_iota(jnp.int32, (tok_dev, HD), 0)
    lane = lax.broadcasted_iota(jnp.int32, (tok_dev, HD), 1)
    early = row < half_tok
    position = jnp.where(
        early, block * half_tok + row, (2 * devices - 1 - block) * half_tok + row - half_tok
    )
    low = lane < HD // 2
    index = jnp.where(low, lane, lane - HD // 2).astype(F32)
    frequency = jnp.exp(index * (-2.0 * math.log(ROPE_BASE) / HD))
    angle = position.astype(F32) * frequency
    sine = jnp.sin(angle)
    return jnp.cos(angle), jnp.where(low, -sine, sine)


def turn(block, cosine, sine):
    wide = block.astype(F32)
    return (wide * cosine + pltpu.roll(wide, HD // 2, 1) * sine).astype(BF16)


def prep_kernel(devices, pairs_hbm, k_hbm, v_hbm, kv_ref, trig_ref, pairs_ref, k_ref, sems):
    tok_dev = k_ref.shape[0]
    width = KVH * HD
    copies = [
        pltpu.make_async_copy(pairs_hbm, pairs_ref, sems.at[0]),
        pltpu.make_async_copy(k_hbm, k_ref, sems.at[1]),
        pltpu.make_async_copy(v_hbm, kv_ref.at[:, width:], sems.at[2]),
    ]
    for copy in copies:
        copy.start()
    copies[0].wait()
    cosine, sine = rotation_tables(pairs_ref[lax.axis_index("seq")], devices, tok_dev)
    trig_ref[:, :HD] = cosine
    trig_ref[:, HD:] = sine
    copies[1].wait()
    for g in range(KVH):
        cols = slice(g * HD, (g + 1) * HD)
        kv_ref[:, cols] = turn(k_ref[:, cols], cosine, sine)
    copies[2].wait()


def prep(pairs, keys, values):
    devices = lax.axis_size("seq")
    tok_dev = keys.shape[0]
    return pl.pallas_call(
        functools.partial(prep_kernel, devices),
        out_shape=(
            jax.ShapeDtypeStruct((tok_dev, 2 * KVH * HD), BF16),
            jax.ShapeDtypeStruct((tok_dev, 2 * HD), F32),
        ),
        in_specs=[HBM_SPEC] * 3,
        out_specs=(VMEM_SPEC,) * 2,
        scratch_shapes=[
            pltpu.SMEM(pairs.shape, jnp.int32),
            pltpu.VMEM(keys.shape, BF16),
            pltpu.SemaphoreType.DMA((3,)),
        ],
        compiler_params=params(8),
        name="prep",
    )(pairs, keys, values)


def turn_kernel(
    devices, q_hbm, pairs_hbm, slots_hbm, trig_ref, turned_ref, info_ref, q_ref, pairs_ref, slots_ref, sems
):
    tok_dev = q_ref.shape[0]
    half_tok = tok_dev // 2
    stride = devices // KVH
    width = GQ * HD
    copies = []
    for g in range(KVH):
        cols = pl.ds(g * width, width)
        copies.append(pltpu.make_async_copy(q_hbm.at[:, cols], q_ref.at[:, cols], sems.at[g]))
    copies.append(pltpu.make_async_copy(pairs_hbm, pairs_ref, sems.at[KVH]))
    copies.append(pltpu.make_async_copy(slots_hbm, slots_ref, sems.at[KVH + 1]))
    for copy in copies:
        copy.start()
    cosine, sine = trig_ref[:, :HD], trig_ref[:, HD:]
    for g in range(KVH):
        copies[g].wait()
        turned = [
            turn(q_ref[:, head * HD : (head + 1) * HD], cosine, sine)
            for head in range(g * GQ, (g + 1) * GQ)
        ]
        for half in range(2):
            part = [t[half * half_tok : (half + 1) * half_tok] for t in turned]
            turned_ref[half, g] = jnp.concatenate(part, axis=0).T
    copies[KVH].wait()
    copies[KVH + 1].wait()
    me = lax.axis_index("seq")
    lane = lax.broadcasted_iota(jnp.int32, (1, devices), 1)
    peers = jnp.zeros((1, devices), jnp.int32)
    for i in range(devices):
        peers = jnp.where(lane == i, pairs_ref[lax.bitwise_xor(me, i)], peers)
    slot = slots_ref[me]
    info_ref[0:1, :] = peers
    info_ref[1:2, :] = jnp.where(lane == 0, slot // stride, slot % stride)


def turn_queries(queries, pairs, slots, trig):
    devices = lax.axis_size("seq")
    rows = GQ * queries.shape[0] // 2
    return pl.pallas_call(
        functools.partial(turn_kernel, devices),
        out_shape=(
            jax.ShapeDtypeStruct((2, KVH, HD, rows), BF16),
            jax.ShapeDtypeStruct((2, devices), jnp.int32),
        ),
        in_specs=[HBM_SPEC] * 3 + [VMEM_SPEC],
        out_specs=(VMEM_SPEC,) * 2,
        scratch_shapes=[
            pltpu.VMEM(queries.shape, BF16),
            pltpu.SMEM(pairs.shape, jnp.int32),
            pltpu.SMEM(slots.shape, jnp.int32),
            pltpu.SemaphoreType.DMA((KVH + 2,)),
        ],
        compiler_params=params(8),
        name="turn",
    )(queries, pairs, slots, trig)


def fold(x):
    return x.reshape(x.shape[0] // 8, 8, x.shape[1])


def spread_max(x):
    for shift in (4, 2, 1):
        x = jnp.maximum(x, pltpu.roll(x, shift, 0))
    return x


def chunk_kernel(devices, offsets, counts, first, last, *refs):
    refs = list(refs)
    info_ref, turned_ref = refs.pop(0), refs.pop(0)
    block_refs = [refs.pop(0) for _ in counts]
    if not first:
        old_refs = [refs.pop(0) for _ in range(3)]
        old_cache_ref = refs.pop(0)
    if last:
        out_hbm, cache_hbm, out_ref, cache_ref, sems = refs
    else:
        new_refs = [refs.pop(0) for _ in range(3)]
        cache_ref = refs.pop(0)

    own = info_ref[0, 0]
    head, phase = info_ref[1, 0], info_ref[1, 1]
    tok_dev = block_refs[0].shape[-2]
    half_tok = tok_dev // 2
    stride = devices // KVH
    rows = GQ * half_tok

    where = []
    for ref, count in zip(block_refs, counts):
        where += [ref.at[i] for i in range(count)] if count else [ref]
    pair_of = [info_ref[0, offset] for offset in offsets]

    def gathered(col, half):
        return jnp.concatenate(
            [w[half * half_tok : (half + 1) * half_tok, pl.ds(col, HD)] for w in where], axis=0
        )

    per_block = half_tok // stride
    peers = len(where)
    out_rows = 2 * per_block * peers
    row = lax.broadcasted_iota(jnp.int32, (out_rows, peers * half_tok), 0)
    lane = lax.broadcasted_iota(jnp.int32, (out_rows, peers * half_tok), 1)
    source = (row // (2 * per_block)) * half_tok + (row % (2 * per_block)) // 2 * stride + phase
    hit = source == lane
    pick_key = jnp.where(hit & (row % 2 == 0), 1.0, 0.0).astype(BF16)
    pick_value = jnp.where(hit & (row % 2 == 1), 1.0, 0.0).astype(BF16)
    key_col = pl.multiple_of(head * HD, HD)
    value_col = pl.multiple_of((KVH + head) * HD, HD)
    if not first:
        cache_ref[...] = old_cache_ref[...]
    for half in range(2):
        picked = jnp.dot(pick_key, gathered(key_col, half), preferred_element_type=F32)
        picked += jnp.dot(pick_value, gathered(value_col, half), preferred_element_type=F32)
        picked = picked.astype(BF16)
        for i, pair in enumerate(pair_of):
            block = pair if half == 0 else 2 * devices - 1 - pair
            cache_ref[block] = picked[i * 2 * per_block : (i + 1) * 2 * per_block]
    copies = []
    if last:
        copies.append(pltpu.make_async_copy(cache_ref, cache_hbm, sems.at[KVH]))
        copies[0].start()

    scale = LOG2E / math.sqrt(HD)
    keys_half = len(where) * half_tok

    row = lax.broadcasted_iota(jnp.int32, (half_tok, HD), 0)
    lane = lax.broadcasted_iota(jnp.int32, (half_tok, HD), 1)

    def key_flags(distance):
        column = jnp.where(distance == 0, row, jnp.where(distance < 0, half_tok, HD))
        return jnp.where(lane == column, 1.0, 0.0).astype(BF16)

    early_flags = jnp.concatenate([key_flags(own - pair) for pair in pair_of], axis=0)
    late_flags = jnp.concatenate([key_flags(pair - own) for pair in pair_of], axis=0)
    blank = jnp.zeros((keys_half, HD), BF16)
    order = lax.broadcasted_iota(jnp.int32, (HD, rows), 0)
    token = lax.broadcasted_iota(jnp.int32, (HD, rows), 1) % half_tok
    barred = jnp.where((order > token) & (order <= half_tok), NEGATIVE, 0.0).astype(BF16)
    ones = jnp.ones((16, 2 * keys_half), BF16)

    def scores_of(g):
        key_early, key_late = gathered(g * HD, 0), gathered(g * HD, 1)
        query_early = jnp.concatenate([turned_ref[0, g], barred], axis=0)
        query_late = jnp.concatenate([turned_ref[1, g], barred], axis=0)
        early = jnp.dot(
            jnp.concatenate([key_early, early_flags], axis=1),
            query_early,
            preferred_element_type=F32,
        )
        late_keys = jnp.concatenate([key_early, key_late], axis=0)
        flags = jnp.concatenate([blank, late_flags], axis=0)
        late = jnp.dot(
            jnp.concatenate([late_keys, flags], axis=1), query_late, preferred_element_type=F32
        )
        return early, late

    def update(half, g, scores, values):
        index = half * KVH + g
        scores = fold(scores)
        top = spread_max(jnp.max(scores, axis=0)) * scale
        if not first:
            old_max = old_refs[0][index]
            top = jnp.maximum(old_max, top)
            factor = jnp.exp2(old_max - top)
        weights = jnp.exp2(scores * scale - top[None]).astype(BF16).reshape(-1, rows)
        both = jnp.dot(values, weights, preferred_element_type=F32)
        mixture, sums = fold(both[:HD]), both[HD : HD + 8]
        if not first:
            sums = old_refs[1][index] * factor + sums
            mixture = fold(old_refs[2][half, g]) * factor[None] + mixture
        if last:
            result = (mixture * (1.0 / sums)[None]).reshape(HD, rows).astype(BF16).T
            for r in range(GQ):
                col = (g * GQ + r) * HD
                out_ref[half * half_tok : (half + 1) * half_tok, col : col + HD] = result[
                    r * half_tok : (r + 1) * half_tok
                ]
        else:
            new_refs[0][index] = top
            new_refs[1][index] = sums
            new_refs[2][half, g] = mixture.reshape(HD, rows)

    scores = [scores_of(g) for g in range(KVH)]
    values = []
    for g in range(KVH):
        value_rows = jnp.concatenate(
            [gathered((KVH + g) * HD, 0), gathered((KVH + g) * HD, 1)], axis=0
        )
        values.append(jnp.concatenate([value_rows.T, ones], axis=0))
    for g in range(KVH):
        update(0, g, scores[g][0], values[g][:, :keys_half])
        update(1, g, scores[g][1], values[g])
        if last:
            cols = pl.ds(g * GQ * HD, GQ * HD)
            copies.append(
                pltpu.make_async_copy(out_ref.at[:, cols], out_hbm.at[:, cols], sems.at[g])
            )
            copies[-1].start()
    for copy in copies:
        copy.wait()


def attend_chunk(info, turned, blocks, offsets, counts, state, last):
    devices = lax.axis_size("seq")
    tok_dev = blocks[0].shape[-2]
    stride = devices // KVH
    rows = GQ * tok_dev // 2
    first = state is None
    operands = [info, turned, *blocks, *(state or ())]
    cache = jax.ShapeDtypeStruct((2 * devices, tok_dev // stride, HD), BF16)
    aliases, scratch = {}, []
    if last:
        out = jax.ShapeDtypeStruct((tok_dev, QH * HD), BF16)
        outs = (out, cache)
        scratch = [
            pltpu.VMEM(out.shape, BF16),
            pltpu.VMEM(cache.shape, BF16),
            pltpu.SemaphoreType.DMA((KVH + 1,)),
        ]
    else:
        small = jax.ShapeDtypeStruct((2 * KVH, 8, rows), F32)
        outs = (small, small, jax.ShapeDtypeStruct((2, KVH, HD, rows), F32), cache)
        if not first:
            aliases = {2 + len(blocks) + i: i for i in range(4)}
    work = len(offsets) * (tok_dev // 2) * rows * KVH * HD
    return pl.pallas_call(
        functools.partial(chunk_kernel, devices, offsets, counts, first, last),
        out_shape=outs,
        in_specs=[VMEM_SPEC] * len(operands),
        out_specs=tuple([HBM_SPEC if last else VMEM_SPEC] * len(outs)),
        scratch_shapes=scratch,
        input_output_aliases=aliases,
        compiler_params=params(24),
        cost_estimate=pl.CostEstimate(flops=12 * work, bytes_accessed=1 << 20, transcendentals=0),
        name="attend",
    )(*operands)


def swap(x, offset):
    devices = lax.axis_size("seq")
    return lax.ppermute(x, "seq", [(s, s ^ offset) for s in range(devices)])


def ring_order(outer):
    direct = [0] + [(1 << k) - 1 for k in range(1, outer.bit_length())]
    return direct + [step for step in range(outer) if step not in direct]


def layout_of(devices):
    cores = 2
    chips = devices // cores
    outer = 1 << -(-(chips.bit_length() - 1) // 2)
    return outer, chips // outer, cores


def whole_step(queries, keys, values, block_pairs, decode_slots):
    devices = lax.axis_size("seq")
    tok_dev = queries.shape[0]
    stride = devices // KVH
    outer, inner, cores = layout_of(devices)

    def hbm(x):
        return pltpu.with_memory_space_constraint(x, pltpu.HBM)

    pairs, slots = hbm(block_pairs), hbm(decode_slots)
    kv, trig = prep(pairs, hbm(keys), hbm(values))
    turned, info = turn_queries(hbm(queries), pairs, slots, trig)
    plane = inner * cores
    far = {0: kv}
    order = ring_order(outer)
    for step in order[1:]:
        full = (1 << step.bit_length()) - 1
        source = 0 if step == full else full
        far[step] = swap(far[source], (step ^ source) * plane)
    state = None
    zeros = (0,) * inner
    for step in order:
        near = [far[step]]
        for y in range(1, inner):
            near.append(swap(far[step], y * cores))
        here = tuple(step * plane + y * cores for y in range(inner))
        there = tuple(i + 1 for i in here)
        if step == order[-1]:
            first, rest = swap(near[0], 1), swap(jnp.stack(near[1:]), 1)
            pieces = [
                (f"a{step}", [*near, first], here + there[:1], (*zeros, 0)),
                ("aend", [rest], there[1:], (inner - 1,)),
            ]
        else:
            pair = swap(jnp.stack(near), 1)
            pieces = [(f"a{step}", [*near, pair], here + there, (*zeros, inner))]
        for name, blocks, offsets, counts in pieces:
            state = attend_chunk(
                info, turned, blocks, offsets, counts, state, name == "aend"
            )
    attended, cache = state
    return attended, cache.reshape(1, tok_dev * devices // stride, 2, HD)


def solution(mesh):
    placed = (
        P(("groups", "seq"), None),
        P(("groups", "seq"), None),
        P(("groups", "seq"), None),
        P("groups"),
        P("groups"),
    )
    return jax.shard_map(
        whole_step,
        mesh=mesh,
        in_specs=placed,
        out_specs=(P(("groups", "seq"), None), P(("groups", "seq"), None, None, None)),
        check_vma=False,
    )
```

```python
import functools
import math

import jax
import jax.numpy as jnp
from jax import lax
from jax.experimental import pallas as pl
from jax.experimental.pallas import tpu as pltpu
from jax.sharding import PartitionSpec as P


HD = 128
KVH = 4
GQ = 8
QH = 32

ROPE_BASE = 500000.0
NEGATIVE = -1e30
LOG2E = math.log2(math.e)

VMEM_SPEC = pl.BlockSpec(memory_space=pltpu.VMEM)
HBM_SPEC = pl.BlockSpec(memory_space=pltpu.HBM)
F32 = jnp.float32
BF16 = jnp.bfloat16


def params(mib):
    return pltpu.CompilerParams(vmem_limit_bytes=mib << 20)


def rotation_tables(block, devices, tok_dev):
    half_tok = tok_dev // 2
    row = lax.broadcasted_iota(jnp.int32, (tok_dev, HD), 0)
    lane = lax.broadcasted_iota(jnp.int32, (tok_dev, HD), 1)
    early = row < half_tok
    position = jnp.where(
        early, block * half_tok + row, (2 * devices - 1 - block) * half_tok + row - half_tok
    )
    low = lane < HD // 2
    index = jnp.where(low, lane, lane - HD // 2).astype(F32)
    frequency = jnp.exp(index * (-2.0 * math.log(ROPE_BASE) / HD))
    angle = position.astype(F32) * frequency
    sine = jnp.sin(angle)
    return jnp.cos(angle), jnp.where(low, -sine, sine)


def turn(block, cosine, sine):
    wide = block.astype(F32)
    return (wide * cosine + pltpu.roll(wide, HD // 2, 1) * sine).astype(BF16)


def prep_kernel(devices, pairs_hbm, k_hbm, v_hbm, kv_ref, trig_ref, pairs_ref, k_ref, sems):
    tok_dev = k_ref.shape[0]
    width = KVH * HD
    copies = [
        pltpu.make_async_copy(pairs_hbm, pairs_ref, sems.at[0]),
        pltpu.make_async_copy(k_hbm, k_ref, sems.at[1]),
        pltpu.make_async_copy(v_hbm, kv_ref.at[:, width:], sems.at[2]),
    ]
    for copy in copies:
        copy.start()
    copies[0].wait()
    cosine, sine = rotation_tables(pairs_ref[lax.axis_index("seq")], devices, tok_dev)
    trig_ref[:, :HD] = cosine
    trig_ref[:, HD:] = sine
    copies[1].wait()
    for g in range(KVH):
        cols = slice(g * HD, (g + 1) * HD)
        kv_ref[:, cols] = turn(k_ref[:, cols], cosine, sine)
    copies[2].wait()


def prep(pairs, keys, values):
    devices = lax.axis_size("seq")
    tok_dev = keys.shape[0]
    return pl.pallas_call(
        functools.partial(prep_kernel, devices),
        out_shape=(
            jax.ShapeDtypeStruct((tok_dev, 2 * KVH * HD), BF16),
            jax.ShapeDtypeStruct((tok_dev, 2 * HD), F32),
        ),
        in_specs=[HBM_SPEC] * 3,
        out_specs=(VMEM_SPEC,) * 2,
        scratch_shapes=[
            pltpu.SMEM(pairs.shape, jnp.int32),
            pltpu.VMEM(keys.shape, BF16),
            pltpu.SemaphoreType.DMA((3,)),
        ],
        compiler_params=params(8),
        name="prep",
    )(pairs, keys, values)


def turn_kernel(
    devices, q_hbm, pairs_hbm, slots_hbm, trig_ref, turned_ref, info_ref, q_ref, pairs_ref, slots_ref, sems
):
    tok_dev = q_ref.shape[0]
    half_tok = tok_dev // 2
    stride = devices // KVH
    width = GQ * HD
    copies = []
    for g in range(KVH):
        cols = pl.ds(g * width, width)
        copies.append(pltpu.make_async_copy(q_hbm.at[:, cols], q_ref.at[:, cols], sems.at[g]))
    copies.append(pltpu.make_async_copy(pairs_hbm, pairs_ref, sems.at[KVH]))
    copies.append(pltpu.make_async_copy(slots_hbm, slots_ref, sems.at[KVH + 1]))
    for copy in copies:
        copy.start()
    cosine, sine = trig_ref[:, :HD], trig_ref[:, HD:]
    for g in range(KVH):
        copies[g].wait()
        turned = [
            turn(q_ref[:, head * HD : (head + 1) * HD], cosine, sine)
            for head in range(g * GQ, (g + 1) * GQ)
        ]
        for half in range(2):
            part = [t[half * half_tok : (half + 1) * half_tok] for t in turned]
            turned_ref[half, g] = jnp.concatenate(part, axis=0).T
    copies[KVH].wait()
    copies[KVH + 1].wait()
    me = lax.axis_index("seq")
    lane = lax.broadcasted_iota(jnp.int32, (1, devices), 1)
    peers = jnp.zeros((1, devices), jnp.int32)
    for i in range(devices):
        peers = jnp.where(lane == i, pairs_ref[lax.bitwise_xor(me, i)], peers)
    slot = slots_ref[me]
    info_ref[0:1, :] = peers
    info_ref[1:2, :] = jnp.where(lane == 0, slot // stride, slot % stride)


def turn_queries(queries, pairs, slots, trig):
    devices = lax.axis_size("seq")
    rows = GQ * queries.shape[0] // 2
    return pl.pallas_call(
        functools.partial(turn_kernel, devices),
        out_shape=(
            jax.ShapeDtypeStruct((2, KVH, HD, rows), BF16),
            jax.ShapeDtypeStruct((2, devices), jnp.int32),
        ),
        in_specs=[HBM_SPEC] * 3 + [VMEM_SPEC],
        out_specs=(VMEM_SPEC,) * 2,
        scratch_shapes=[
            pltpu.VMEM(queries.shape, BF16),
            pltpu.SMEM(pairs.shape, jnp.int32),
            pltpu.SMEM(slots.shape, jnp.int32),
            pltpu.SemaphoreType.DMA((KVH + 2,)),
        ],
        compiler_params=params(8),
        name="turn",
    )(queries, pairs, slots, trig)


def fold(x):
    return x.reshape(x.shape[0] // 8, 8, x.shape[1])


def spread_max(x):
    for shift in (4, 2, 1):
        x = jnp.maximum(x, pltpu.roll(x, shift, 0))
    return x


def chunk_kernel(devices, offsets, counts, first, last, *refs):
    refs = list(refs)
    info_ref, turned_ref = refs.pop(0), refs.pop(0)
    block_refs = [refs.pop(0) for _ in counts]
    if not first:
        old_refs = [refs.pop(0) for _ in range(3)]
        old_cache_ref = refs.pop(0)
    if last:
        out_hbm, cache_hbm, out_ref, cache_ref, sems = refs
    else:
        new_refs = [refs.pop(0) for _ in range(3)]
        cache_ref = refs.pop(0)

    own = info_ref[0, 0]
    head, phase = info_ref[1, 0], info_ref[1, 1]
    tok_dev = block_refs[0].shape[-2]
    half_tok = tok_dev // 2
    stride = devices // KVH
    rows = GQ * half_tok

    where = []
    for ref, count in zip(block_refs, counts):
        where += [ref.at[i] for i in range(count)] if count else [ref]
    pair_of = [info_ref[0, offset] for offset in offsets]

    def gathered(col, half):
        return jnp.concatenate(
            [w[half * half_tok : (half + 1) * half_tok, pl.ds(col, HD)] for w in where], axis=0
        )

    per_block = half_tok // stride
    peers = len(where)
    out_rows = 2 * per_block * peers
    row = lax.broadcasted_iota(jnp.int32, (out_rows, peers * half_tok), 0)
    lane = lax.broadcasted_iota(jnp.int32, (out_rows, peers * half_tok), 1)
    source = (row // (2 * per_block)) * half_tok + (row % (2 * per_block)) // 2 * stride + phase
    hit = source == lane
    pick_key = jnp.where(hit & (row % 2 == 0), 1.0, 0.0).astype(BF16)
    pick_value = jnp.where(hit & (row % 2 == 1), 1.0, 0.0).astype(BF16)
    key_col = pl.multiple_of(head * HD, HD)
    value_col = pl.multiple_of((KVH + head) * HD, HD)
    if not first:
        cache_ref[...] = old_cache_ref[...]
    for half in range(2):
        picked = jnp.dot(pick_key, gathered(key_col, half), preferred_element_type=F32)
        picked += jnp.dot(pick_value, gathered(value_col, half), preferred_element_type=F32)
        picked = picked.astype(BF16)
        for i, pair in enumerate(pair_of):
            block = pair if half == 0 else 2 * devices - 1 - pair
            cache_ref[block] = picked[i * 2 * per_block : (i + 1) * 2 * per_block]
    copies = []
    if last:
        copies.append(pltpu.make_async_copy(cache_ref, cache_hbm, sems.at[KVH]))
        copies[0].start()

    scale = LOG2E / math.sqrt(HD)
    keys_half = len(where) * half_tok

    row = lax.broadcasted_iota(jnp.int32, (half_tok, HD), 0)
    lane = lax.broadcasted_iota(jnp.int32, (half_tok, HD), 1)

    def key_flags(distance):
        column = jnp.where(distance == 0, row, jnp.where(distance < 0, half_tok, HD))
        return jnp.where(lane == column, 1.0, 0.0).astype(BF16)

    early_flags = jnp.concatenate([key_flags(own - pair) for pair in pair_of], axis=0)
    late_flags = jnp.concatenate([key_flags(pair - own) for pair in pair_of], axis=0)
    blank = jnp.zeros((keys_half, HD), BF16)
    order = lax.broadcasted_iota(jnp.int32, (HD, rows), 0)
    token = lax.broadcasted_iota(jnp.int32, (HD, rows), 1) % half_tok
    barred = jnp.where((order > token) & (order <= half_tok), NEGATIVE, 0.0).astype(BF16)
    ones = jnp.ones((16, 2 * keys_half), BF16)

    def masked_scores_of(g):
        key_early, key_late = gathered(g * HD, 0), gathered(g * HD, 1)
        ahead = lax.broadcasted_iota(jnp.int32, (half_tok, rows), 0) - (
            lax.broadcasted_iota(jnp.int32, (half_tok, rows), 1) % half_tok
        )
        early_ok = jnp.concatenate([ahead <= half_tok * (own - pair) for pair in pair_of], axis=0)
        late_ok = jnp.concatenate([ahead <= half_tok * (pair - own) for pair in pair_of], axis=0)
        early = jnp.dot(key_early, turned_ref[0, g], preferred_element_type=F32)
        late = jnp.dot(
            jnp.concatenate([key_early, key_late], axis=0),
            turned_ref[1, g],
            preferred_element_type=F32,
        )
        late_half = jnp.where(late_ok, late[keys_half:], NEGATIVE)
        return (
            jnp.where(early_ok, early, NEGATIVE),
            jnp.concatenate([late[:keys_half], late_half], axis=0),
        )

    def scores_of(g):
        key_early, key_late = gathered(g * HD, 0), gathered(g * HD, 1)
        query_early = jnp.concatenate([turned_ref[0, g], barred], axis=0)
        query_late = jnp.concatenate([turned_ref[1, g], barred], axis=0)
        early = jnp.dot(
            jnp.concatenate([key_early, early_flags], axis=1),
            query_early,
            preferred_element_type=F32,
        )
        late_keys = jnp.concatenate([key_early, key_late], axis=0)
        flags = jnp.concatenate([blank, late_flags], axis=0)
        late = jnp.dot(
            jnp.concatenate([late_keys, flags], axis=1), query_late, preferred_element_type=F32
        )
        return early, late

    def update(half, g, scores, values):
        index = half * KVH + g
        scores = fold(scores)
        top = spread_max(jnp.max(scores, axis=0)) * scale
        if not first:
            old_max = old_refs[0][index]
            top = jnp.maximum(old_max, top)
            factor = jnp.exp2(old_max - top)
        weights = jnp.exp2(scores * scale - top[None]).astype(BF16).reshape(-1, rows)
        both = jnp.dot(values, weights, preferred_element_type=F32)
        mixture, sums = fold(both[:HD]), both[HD : HD + 8]
        if not first:
            sums = old_refs[1][index] * factor + sums
            mixture = fold(old_refs[2][half, g]) * factor[None] + mixture
        if last:
            result = (mixture * (1.0 / sums)[None]).reshape(HD, rows).astype(BF16).T
            for r in range(GQ):
                col = (g * GQ + r) * HD
                out_ref[half * half_tok : (half + 1) * half_tok, col : col + HD] = result[
                    r * half_tok : (r + 1) * half_tok
                ]
        else:
            new_refs[0][index] = top
            new_refs[1][index] = sums
            new_refs[2][half, g] = mixture.reshape(HD, rows)

    score = masked_scores_of if last else scores_of
    scores = [score(g) for g in range(KVH)]
    values = []
    for g in range(KVH):
        value_rows = jnp.concatenate(
            [gathered((KVH + g) * HD, 0), gathered((KVH + g) * HD, 1)], axis=0
        )
        values.append(jnp.concatenate([value_rows.T, ones], axis=0))
    for g in range(KVH):
        update(0, g, scores[g][0], values[g][:, :keys_half])
        update(1, g, scores[g][1], values[g])
        if last:
            cols = pl.ds(g * GQ * HD, GQ * HD)
            copies.append(
                pltpu.make_async_copy(out_ref.at[:, cols], out_hbm.at[:, cols], sems.at[g])
            )
            copies[-1].start()
    for copy in copies:
        copy.wait()


def attend_chunk(info, turned, blocks, offsets, counts, state, last):
    devices = lax.axis_size("seq")
    tok_dev = blocks[0].shape[-2]
    stride = devices // KVH
    rows = GQ * tok_dev // 2
    first = state is None
    operands = [info, turned, *blocks, *(state or ())]
    cache = jax.ShapeDtypeStruct((2 * devices, tok_dev // stride, HD), BF16)
    aliases, scratch = {}, []
    if last:
        out = jax.ShapeDtypeStruct((tok_dev, QH * HD), BF16)
        outs = (out, cache)
        scratch = [
            pltpu.VMEM(out.shape, BF16),
            pltpu.VMEM(cache.shape, BF16),
            pltpu.SemaphoreType.DMA((KVH + 1,)),
        ]
    else:
        small = jax.ShapeDtypeStruct((2 * KVH, 8, rows), F32)
        outs = (small, small, jax.ShapeDtypeStruct((2, KVH, HD, rows), F32), cache)
        if not first:
            aliases = {2 + len(blocks) + i: i for i in range(4)}
    work = len(offsets) * (tok_dev // 2) * rows * KVH * HD
    return pl.pallas_call(
        functools.partial(chunk_kernel, devices, offsets, counts, first, last),
        out_shape=outs,
        in_specs=[VMEM_SPEC] * len(operands),
        out_specs=tuple([HBM_SPEC if last else VMEM_SPEC] * len(outs)),
        scratch_shapes=scratch,
        input_output_aliases=aliases,
        compiler_params=params(24),
        cost_estimate=pl.CostEstimate(flops=12 * work, bytes_accessed=1 << 20, transcendentals=0),
        name="attend",
    )(*operands)


def swap(x, offset):
    devices = lax.axis_size("seq")
    return lax.ppermute(x, "seq", [(s, s ^ offset) for s in range(devices)])


def ring_order(outer):
    direct = [0] + [(1 << k) - 1 for k in range(1, outer.bit_length())]
    return direct + [step for step in range(outer) if step not in direct]


def layout_of(devices):
    cores = 2
    chips = devices // cores
    outer = 1 << -(-(chips.bit_length() - 1) // 2)
    return outer, chips // outer, cores


def whole_step(queries, keys, values, block_pairs, decode_slots):
    devices = lax.axis_size("seq")
    tok_dev = queries.shape[0]
    stride = devices // KVH
    outer, inner, cores = layout_of(devices)

    def hbm(x):
        return pltpu.with_memory_space_constraint(x, pltpu.HBM)

    pairs, slots = hbm(block_pairs), hbm(decode_slots)
    kv, trig = prep(pairs, hbm(keys), hbm(values))
    turned, info = turn_queries(hbm(queries), pairs, slots, trig)
    plane = inner * cores
    far = {0: kv}
    order = ring_order(outer)
    for step in order[1:]:
        full = (1 << step.bit_length()) - 1
        source = 0 if step == full else full
        far[step] = swap(far[source], (step ^ source) * plane)
    state = None
    zeros = (0,) * inner
    for step in order:
        near = [far[step]]
        for y in range(1, inner):
            near.append(swap(far[step], y * cores))
        here = tuple(step * plane + y * cores for y in range(inner))
        there = tuple(i + 1 for i in here)
        if step == order[-1]:
            first, rest = swap(near[0], 1), swap(jnp.stack(near[1:]), 1)
            pieces = [
                (f"a{step}", [*near, first], here + there[:1], (*zeros, 0)),
                ("aend", [rest], there[1:], (inner - 1,)),
            ]
        else:
            pair = swap(jnp.stack(near), 1)
            pieces = [(f"a{step}", [*near, pair], here + there, (*zeros, inner))]
        for name, blocks, offsets, counts in pieces:
            state = attend_chunk(
                info, turned, blocks, offsets, counts, state, name == "aend"
            )
    attended, cache = state
    return attended, cache.reshape(1, tok_dev * devices // stride, 2, HD)


def solution(mesh):
    placed = (
        P(("groups", "seq"), None),
        P(("groups", "seq"), None),
        P(("groups", "seq"), None),
        P("groups"),
        P("groups"),
    )
    return jax.shard_map(
        whole_step,
        mesh=mesh,
        in_specs=placed,
        out_specs=(P(("groups", "seq"), None), P(("groups", "seq"), None, None, None)),
        check_vma=False,
    )
```
